512 devices in a mesh: rows: 64 (over z, y), cent: 8 (over x, core).
Axes of the slice: x: 4, y: 8, z: 8, core: 2. Of those that a mesh axis runs over, the one named last changes fastest.
Arguments:
- points: bfloat16 [65536, 1024], P('rows'), may hold values from -8 to 8
- centroids: bfloat16 [4096, 1024], P('cent'), may hold values from -8 to 8
- assign: int32 [65536], P('rows'), may hold values from 0 to 4095, as said below
Outputs:
- nearest: float32 [2, 65536], P(None, 'rows')
- updated: bfloat16 [4096, 1024], P('cent')
The draws below stay inside these ranges and needn't reach their ends.
Inputs may be any that keep to these rules, and one draw needn't show every extreme that they name: `assign`: split the points into aligned blocks of 1024 and the centroids into aligned groups of 8 consecutive ones: in each block at most 4 points are assigned into any one group, and in every block some group takes exactly 4 of them.
All inputs are finite; a program needn't handle non-finite values.
Results may differ from the reference program's by a relative error of at most 0.001.
Values may be sent and summed in bfloat16 or wider, within the bound.
A program may use at most 64 MiB of HBM per device.

```python
import jax
import jax.numpy as jnp
from jax import lax

D = 1024
K = 4096
PTS_DEV = 1024
P_SIZE = 65536
GROUPS = 512
SHARE = 8
CAP = 4


def centroid_field(key):
    key_dir, key_len = jax.random.split(jax.random.fold_in(key, 23), 2)
    raw = jax.random.normal(key_dir, (K, D), jnp.float32)
    length = jax.random.uniform(key_len, (K, 1), jnp.float32, 0.97, 1.03)
    return raw * (length * jnp.sqrt(jnp.float32(D)) / jnp.sqrt(jnp.sum(raw * raw, axis=1, keepdims=True)))


def draw_centroids(key, part):
    return centroid_field(key).astype(jnp.bfloat16)


def draw_points(key, part):
    key_val, key_scale, key_pick = jax.random.split(jax.random.fold_in(key, 37), 3)
    cents = centroid_field(key).astype(jnp.bfloat16).astype(jnp.float32)
    picks = jax.random.randint(key_pick, (P_SIZE,), 0, K)
    noise = jax.random.normal(key_val, (P_SIZE, D), jnp.float32)
    low, high = (0.2, 1.5)
    logs = jax.random.uniform(key_scale, (P_SIZE, 1), jnp.float32, jnp.log(low), jnp.log(high))
    scaled = jnp.clip(jnp.exp(logs) * cents[picks] + 0.3 * noise, -8.0, 8.0)
    return scaled.astype(jnp.bfloat16)


def draw_assign(key, part):
    blocks_total = P_SIZE // PTS_DEV
    key_block, key_order, key_shuffle, key_offset = jax.random.split(jax.random.fold_in(key, 11), 4)
    picked = jax.random.randint(key_block, (blocks_total,), 0, GROUPS)
    slot_group = jnp.repeat(jnp.arange(GROUPS, dtype=jnp.int32), CAP)

    def one_block(index):
        order = jax.random.permutation(jax.random.fold_in(key_order, index), GROUPS * CAP).astype(jnp.int32)
        forced = slot_group == picked[index]
        score = jnp.where(forced, order - GROUPS * CAP, order)
        chosen = slot_group[jnp.argsort(score, stable=True)[:PTS_DEV]]
        mixing = jax.random.permutation(jax.random.fold_in(key_shuffle, index), PTS_DEV)
        return chosen[mixing]
    groups_all = jax.vmap(one_block)(jnp.arange(blocks_total, dtype=jnp.int32))
    offsets = jax.random.randint(key_offset, (blocks_total, PTS_DEV), 0, SHARE)
    return (groups_all * SHARE + offsets).reshape(P_SIZE).astype(jnp.int32)


def setup_inputs(seed: int = 0) -> dict:
    arg_keys = jax.random.split(jax.random.key(seed), 4)
    return {
        "points": draw_points(jax.random.fold_in(arg_keys[3], 71), 0),
        "centroids": draw_centroids(jax.random.fold_in(arg_keys[3], 71), 0),
        "assign": draw_assign(jax.random.fold_in(arg_keys[3], 71), 0),
    }


def smallest(points, pnorm, cents):
    cnorm = jnp.sum(jnp.square(cents.astype(jnp.float32)), axis=1)
    size = P_SIZE
    if P_SIZE % 1024 == 0:
        size = 1024

    def one_block(pair):
        block, norms = pair
        dots = lax.dot_general(block, cents, (((1,), (1,)), ((), ())), preferred_element_type=jnp.float32)
        return jnp.min((norms[:, None] - 2.0 * dots + cnorm[None, :]) / D, axis=1)

    result = lax.map(one_block, (points.reshape(P_SIZE // size, size, D), pnorm.reshape(P_SIZE // size, size)))
    return result.reshape(P_SIZE)


def reference(points, centroids, assign):
    wide = points.astype(jnp.float32)
    pnorm = jnp.sum(jnp.square(wide), axis=1)
    first = smallest(points, pnorm, centroids)
    sums = jax.ops.segment_sum(wide, assign, num_segments=K)
    counts = jax.ops.segment_sum(jnp.ones((P_SIZE,), jnp.float32), assign, num_segments=K)
    updated = ((sums + centroids.astype(jnp.float32)) / (counts[:, None] + 1.0)).astype(jnp.bfloat16)
    second = smallest(points, pnorm, updated)
    return jnp.stack([first, second]), updated
```

```python
import functools

import jax
import jax.numpy as jnp
from jax import lax
from jax.experimental import pallas as pl
from jax.experimental.pallas import tpu as pltpu
from jax.sharding import PartitionSpec as P

MESH = pl.DeviceIdType.MESH
F32 = jnp.float32
BF16 = jnp.bfloat16
RING = 8
HALF = RING // 2
SHARE = 8
CAP = 4
LANES = 128
NT = (((1,), (1,)), ((), ()))
ORDER = (4, 3, 5, 2, 6, 1, 7)


def iota(shape, dim):
    return lax.broadcasted_iota(jnp.int32, shape, dim)


def kernel(
    points_hbm, cents_hbm, assign_ref, nearest_ref, updated_hbm,
    pts, cents, place, slots, labels, got, got_labels, part, parts, new, best, bests, pnorm,
    local_sem, out_sem, s1_send, s1_recv, l1_send, l1_recv, s2_send, s2_recv,
    g1_send, g1_recv, g2_send, g2_recv, c_send, c_recv,
):
    n_pts, width = points_hbm.shape
    blocks = n_pts // LANES
    row = lax.axis_index("rows")
    cent = lax.axis_index("cent")
    z = row // RING
    y = row % RING
    par = (z + y) % 2
    pos = (y, z)
    n_cent = bests.shape[1]

    def at(route, p):
        return z * RING + p if route == 0 else p * RING + y

    load_pts = pltpu.make_async_copy(points_hbm, pts, local_sem.at[0])
    load_cents = pltpu.make_async_copy(cents_hbm, cents, local_sem.at[1])
    load_pts.start()
    load_cents.start()

    barrier = pltpu.get_barrier_semaphore()
    for route in (0, 1):
        for i in ORDER:
            pl.semaphore_signal(
                barrier, inc=1, device_id={"rows": at(route, (pos[route] + i) % RING)}, device_id_type=MESH
            )
    for i in range(1, n_cent):
        pl.semaphore_signal(barrier, inc=1, device_id={"cent": (cent + i) % n_cent}, device_id_type=MESH)

    rel = assign_ref[...] - cent * (RING * RING * SHARE)
    inside = (rel >= 0) & (rel < RING * RING * SHARE)
    owner = jnp.where(inside, rel // SHARE, -1)
    label = jnp.where(inside, rel % SHARE + 1, 0).astype(F32)
    oz = owner // RING
    oy = owner % RING
    kind = (oz + oy) % 2
    prim = jnp.where(kind == 0, oy, oz)
    sec = jnp.where(kind == 0, oz, oy) // 2
    me_lane = jnp.where(kind == 0, y, z) * (HALF * CAP)

    groups = iota((RING * RING, LANES), 0)
    hots = [(groups == owner[b : b + 1, :]).astype(F32) for b in range(blocks)]
    upper = (iota((LANES, LANES), 0) < iota((LANES, LANES), 1)).astype(BF16)
    within = jnp.dot(
        jnp.concatenate(hots, axis=0).astype(BF16), upper, preferred_element_type=F32
    )
    carry = jnp.zeros((RING * RING, 1), F32)
    marks, spots = [], []
    for b in range(blocks):
        before = within[b * RING * RING : (b + 1) * RING * RING] + carry
        rank = jnp.sum(hots[b] * before, axis=0, keepdims=True).astype(jnp.int32)
        carry = carry + jnp.sum(hots[b], axis=1, keepdims=True)
        ins, knd, prm = inside[b : b + 1, :], kind[b : b + 1, :], prim[b : b + 1, :]
        spot = sec[b : b + 1, :] * CAP + rank
        slot = jnp.where(ins, (knd * RING + prm) * (HALF * CAP) + spot, -1)
        columns = slice(b * LANES, (b + 1) * LANES)
        place[:, columns] = (iota((place.shape[0], LANES), 0) == slot).astype(F32).astype(BF16)
        marks.append(
            jnp.where(
                iota((2 * RING, LANES), 0) == jnp.where(ins, knd * RING + prm, -1), label[b : b + 1, :], 0.0
            )
        )
        spots.append((iota((LANES, LANES), 0) == me_lane[b : b + 1, :] + spot).astype(F32))
    mine = lax.dot_general(
        jnp.concatenate(marks, axis=1).astype(BF16),
        jnp.concatenate(spots, axis=1).astype(BF16),
        NT,
        preferred_element_type=F32,
    )
    for d in range(2 * RING):
        labels[d] = mine[d : d + 1, :]

    load_pts.wait()
    tile = 256

    def place_tile(i, _):
        columns = pl.ds(pl.multiple_of(i * tile, tile), tile)
        rows = jnp.dot(place[...], pts[:, columns], preferred_element_type=F32).astype(BF16)
        slots[:, :, columns] = rows.reshape(2 * RING, HALF * CAP, tile)
        return 0

    lax.fori_loop(0, width // tile, place_tile, 0)

    pl.semaphore_wait(barrier, 2 * (RING - 1) + n_cent - 1)

    def stage1(route, i):
        to = (pos[route] + i) % RING
        who = {"rows": at(route, to)}
        return (
            pltpu.make_async_remote_copy(
                labels.at[route * RING + to], got_labels.at[route, pos[route]],
                l1_send.at[route, i], l1_recv.at[route, i], who, MESH,
            ),
            pltpu.make_async_remote_copy(
                slots.at[route * RING + to], got.at[route, pos[route]],
                s1_send.at[route, i], s1_recv.at[route, i], who, MESH,
            ),
        )

    for i in ORDER:
        for route in (0, 1):
            for copy in stage1(route, i):
                copy.start()
    for route in (0, 1):
        got_labels[route, pos[route]] = labels[route * RING + pos[route]]
        got[route, pos[route]] = slots[route * RING + pos[route]]

    load_cents.wait()
    chunk = 8

    def smallest(block, low):
        dots = lax.dot_general(block, pts[...], NT, preferred_element_type=F32)
        wide = block.astype(F32)
        norm = jnp.sum(wide * wide, axis=1, keepdims=True)
        return jnp.minimum(low, jnp.min(norm - 2.0 * dots, axis=0, keepdims=True))

    def first_tile(i, low):
        block = cents[pl.ds(i * chunk, chunk)].reshape(chunk * SHARE, width)
        return smallest(block, low)

    none = jnp.full((1, n_pts), jnp.inf, F32)
    best[0] = lax.fori_loop(0, RING * RING // chunk, first_tile, none)
    bests[0, cent] = best[0]

    def norm_tile(i, _):
        rows = pl.ds(pl.multiple_of(i * LANES, LANES), LANES)
        wide = pts[rows, :].astype(F32)
        total = jnp.sum(wide * wide, axis=1, keepdims=True)
        pnorm[:, rows] = jnp.transpose(jnp.broadcast_to(total, (LANES, LANES)))[0:1, :]
        return 0

    lax.fori_loop(0, blocks, norm_tile, 0)

    def across(which, i):
        return pltpu.make_async_remote_copy(
            best.at[which], bests.at[which, cent], c_send.at[which, i], c_recv.at[which, i],
            {"cent": (cent + i) % n_cent}, MESH,
        )

    for route in (0, 1):
        for i in ORDER:
            for copy in stage1(route, i):
                copy.wait_recv()

    def stage2(route, j):
        to = 2 * j + (pos[route] + route) % 2
        me = pos[1 - route]
        return to == me, pltpu.make_async_remote_copy(
            part.at[route, j], parts.at[me],
            s2_send.at[route, j], s2_recv.at[me],
            {"rows": at(1 - route, to)}, MESH,
        )

    for route in (0, 1):
        names = jnp.sum(got_labels[route], axis=0)
        lane = iota((1, LANES), 1)
        target = jnp.where(names > 0.0, ((lane % (HALF * CAP)) // CAP * SHARE).astype(F32) + names - 1.0, -1.0)
        chosen = (iota((HALF * SHARE, LANES), 0).astype(F32) == target).astype(F32)
        counts = jnp.sum(chosen, axis=1, keepdims=True)
        arrived = got[route].reshape(RING * HALF * CAP, width)
        sums = jnp.dot(chosen.astype(BF16), arrived, preferred_element_type=F32)
        part[route, :, :, 0:width] = sums.reshape(HALF, SHARE, width)
        part[route, :, :, width : width + LANES] = jnp.broadcast_to(counts, (HALF * SHARE, LANES)).reshape(
            HALF, SHARE, LANES
        )
        for j in range(HALF):
            mine_too, copy = stage2(route, j)

            @pl.when(jnp.logical_not(mine_too))
            def _():
                copy.start()

            @pl.when(mine_too)
            def _():
                parts[pos[1 - route]] = part[route, j]

    for i in range(1, n_cent):
        across(0, i).start()

    mine_along = jnp.where(par == 0, z, y)
    mine_across = jnp.where(par == 0, y, z)
    for i in range(1, RING):
        src = (mine_along + i) % RING
        pltpu.make_async_remote_copy(
            part.at[0, 0], parts.at[src], s2_send.at[0, 0], s2_recv.at[src], {"rows": row}, MESH
        ).wait_recv()
    total = parts[0]
    for i in range(1, RING):
        total = total + parts[i]
    fresh = (total[:, 0:width] + cents[row].astype(F32)) / (total[:, width : width + 1] + 1.0)
    new[par, mine_across, mine_along // 2] = fresh.astype(BF16)

    def gather1(i):
        to = (mine_along + i) % RING
        who = jnp.where(par == 0, to * RING + y, z * RING + to)
        spot = new.at[par, mine_across, mine_along // 2]
        return pltpu.make_async_remote_copy(
            spot, spot, g1_send.at[i], g1_recv.at[par, mine_along // 2], {"rows": who}, MESH
        )

    for i in ORDER:
        gather1(i).start()

    def ring(route, s, d, j):
        sign = 1 - 2 * d
        spot = new.at[route, (pos[route] - sign * (s - 1)) % RING, j]
        return pltpu.make_async_remote_copy(
            spot, spot, g2_send.at[route, d, s, j], g2_recv.at[route, d, s, j],
            {"rows": at(route, (pos[route] + sign) % RING)}, MESH,
        )

    def used(s, d, j):
        return s < HALF or (j < HALF // 2) == (d == 0)

    for j in range(HALF):
        for route in (0, 1):
            src = 2 * j + (pos[route] + route) % 2

            @pl.when(src != pos[1 - route])
            def _():
                spot = new.at[route, pos[route], j]
                pltpu.make_async_remote_copy(
                    spot, spot, g1_send.at[0], g1_recv.at[route, j], {"rows": row}, MESH
                ).wait_recv()

            for d in (0, 1):
                ring(route, 1, d, j).start()
    for s in range(2, HALF + 2):
        for j in range(HALF):
            for route in (0, 1):
                for d in (0, 1):
                    if used(s - 1, d, j):
                        ring(route, s - 1, d, j).wait_recv()
                    if s <= HALF and used(s, d, j):
                        ring(route, s, d, j).start()

    def store(route, p):
        if route == 0:
            return pltpu.make_async_copy(
                new.at[0, p], updated_hbm.at[:, p % 2, p // 2, p % 2], out_sem.at[0, p]
            )
        return pltpu.make_async_copy(new.at[1, p], updated_hbm.at[p // 2, p % 2, :, 1 - p % 2], out_sem.at[1, p])

    for p in range(RING):
        for route in (0, 1):
            store(route, p).start()

    def second_tile(i, low):
        for route in (0, 1):
            block = new[route, pl.ds(i * 2, 2)].reshape(2 * HALF * SHARE, width)
            low = smallest(block, low)
        return low

    best[1] = lax.fori_loop(0, HALF, second_tile, none)
    for i in range(1, n_cent):
        across(1, i).start()
    bests[1, cent] = best[1]
    for which in (0, 1):
        for i in range(1, n_cent):
            across(which, i).wait_recv()
        low = bests[which, 0]
        for i in range(1, n_cent):
            low = jnp.minimum(low, bests[which, i])
        nearest_ref[which : which + 1, :] = (pnorm[...] + low) / width

    for route in (0, 1):
        for i in ORDER:
            for copy in stage1(route, i):
                copy.wait_send()
        for j in range(HALF):
            mine_too, copy = stage2(route, j)

            @pl.when(jnp.logical_not(mine_too))
            def _():
                copy.wait_send()

        for p in range(RING):
            store(route, p).wait()
    for i in ORDER:
        gather1(i).wait_send()
    for s in range(1, HALF + 1):
        for j in range(HALF):
            for route in (0, 1):
                for d in (0, 1):
                    if used(s, d, j):
                        ring(route, s, d, j).wait_send()
    for which in (0, 1):
        for i in range(1, n_cent):
            across(which, i).wait_send()


def solution(mesh):
    n_cent = mesh.shape["cent"]

    def per_device(points, centroids, assign):
        n_pts, width = points.shape
        dma = pltpu.SemaphoreType.DMA
        nearest, updated = pl.pallas_call(
            kernel,
            out_shape=(
                jax.ShapeDtypeStruct((2, n_pts), F32),
                jax.ShapeDtypeStruct((HALF, 2, HALF, 2, SHARE, width), BF16),
            ),
            in_specs=[
                pl.BlockSpec(memory_space=pl.ANY),
                pl.BlockSpec(memory_space=pl.ANY),
                pl.BlockSpec(memory_space=pltpu.VMEM),
            ],
            out_specs=(pl.BlockSpec(memory_space=pltpu.VMEM), pl.BlockSpec(memory_space=pl.ANY)),
            scratch_shapes=[
                pltpu.VMEM((n_pts, width), BF16),
                pltpu.VMEM((RING * RING, SHARE, width), BF16),
                pltpu.VMEM((2 * RING * HALF * CAP, n_pts), BF16),
                pltpu.VMEM((2 * RING, HALF * CAP, width), BF16),
                pltpu.VMEM((2 * RING, 1, LANES), F32),
                pltpu.VMEM((2, RING, HALF * CAP, width), BF16),
                pltpu.VMEM((2, RING, 1, LANES), F32),
                pltpu.VMEM((2, HALF, SHARE, width + LANES), F32),
                pltpu.VMEM((RING, SHARE, width + LANES), F32),
                pltpu.VMEM((2, RING, HALF, SHARE, width), BF16),
                pltpu.VMEM((2, 1, n_pts), F32),
                pltpu.VMEM((2, n_cent, 1, n_pts), F32),
                pltpu.VMEM((1, n_pts), F32),
                dma((2,)),
                dma((2, RING)),
                dma((2, RING)),
                dma((2, RING)),
                dma((2, RING)),
                dma((2, RING)),
                dma((2, HALF)),
                dma((RING,)),
                dma((RING,)),
                dma((2, HALF)),
                dma((2, 2, HALF + 1, HALF)),
                dma((2, 2, HALF + 1, HALF)),
                dma((2, n_cent)),
                dma((2, n_cent)),
            ],
            compiler_params=pltpu.CompilerParams(
                collective_id=0, has_side_effects=True, vmem_limit_bytes=60 * 1024 * 1024
            ),
        )(
            points,
            centroids.reshape(RING * RING, SHARE, width),
            assign.reshape(n_pts // LANES, LANES),
        )
        return nearest, updated.reshape(RING * RING * SHARE, width)

    return jax.shard_map(
        per_device,
        mesh=mesh,
        in_specs=(P("rows", None), P("cent", None), P("rows")),
        out_specs=(P(None, "rows"), P("cent", None)),
        check_vma=False,
    )
```

```python
import functools

import jax
import jax.numpy as jnp
from jax import lax
from jax.experimental import pallas as pl
from jax.experimental.pallas import tpu as pltpu
from jax.sharding import PartitionSpec as P

MESH = pl.DeviceIdType.MESH
F32 = jnp.float32
BF16 = jnp.bfloat16
RING = 8
HALF = RING // 2
SHARE = 8
CAP = 4
LANES = 128
NT = (((1,), (1,)), ((), ()))
ORDER = (4, 3, 5, 2, 6, 1, 7)
ONE, TWO, THREE, FAR = range(4)
HOPS = ((1, 0), (2, 0), (1, 2), (2, 2))
WAVE = sorted(((s, q) for s in range(2) for q in range(HALF)), key=lambda e: 10 * e[1] + 33 * e[0])


def iota(shape, dim):
    return lax.broadcasted_iota(jnp.int32, shape, dim)


def kernel(
    points_hbm, cents_hbm, assign_hbm, new, bests, pnorm,
    assigned, pts, cents, place, slots, labels, got, got_labels, part, parts, best,
    local_sem, s1_send, s1_recv, l1_send, l1_recv, s2_send, s2_recv,
    g1_send, g1_recv, g2_send, g2_recv, c_send, c_recv,
):
    n_pts, width = points_hbm.shape
    blocks = n_pts // LANES
    row = lax.axis_index("rows")
    cent = lax.axis_index("cent")
    z = row // RING
    y = row % RING
    par = (z + y) % 2
    pos = (y, z)
    n_cent = bests.shape[1]

    def at(route, p):
        return z * RING + p if route == 0 else p * RING + y

    load_assign = pltpu.make_async_copy(assign_hbm, assigned, local_sem.at[2])
    load_assign.start()
    load_pts = pltpu.make_async_copy(points_hbm, pts, local_sem.at[0])
    load_cents = pltpu.make_async_copy(cents_hbm, cents, local_sem.at[1])
    load_pts.start()
    load_cents.start()

    barrier = pltpu.get_barrier_semaphore()
    for route in (0, 1):
        for i in ORDER:
            pl.semaphore_signal(
                barrier, inc=1, device_id={"rows": at(route, (pos[route] + i) % RING)}, device_id_type=MESH
            )
    for i in range(1, n_cent):
        pl.semaphore_signal(barrier, inc=1, device_id={"cent": (cent + i) % n_cent}, device_id_type=MESH)

    load_assign.wait()
    rel = assigned[...] - cent * (RING * RING * SHARE)
    inside = (rel >= 0) & (rel < RING * RING * SHARE)
    owner = jnp.where(inside, rel // SHARE, -1)
    label = jnp.where(inside, rel % SHARE + 1, 0).astype(F32)
    oz = owner // RING
    oy = owner % RING
    kind = (oz + oy) % 2
    prim = jnp.where(kind == 0, oy, oz)
    sec = jnp.where(kind == 0, oz, oy) // 2
    me_lane = jnp.where(kind == 0, y, z) * (HALF * CAP)

    groups = iota((RING * RING, LANES), 0)
    hots = [(groups == owner[b : b + 1, :]).astype(F32) for b in range(blocks)]
    upper = (iota((LANES, LANES), 0) < iota((LANES, LANES), 1)).astype(BF16)
    within = jnp.dot(
        jnp.concatenate(hots, axis=0).astype(BF16), upper, preferred_element_type=F32
    )
    carry = jnp.zeros((RING * RING, 1), F32)
    marks, spots = [], []
    for b in range(blocks):
        before = within[b * RING * RING : (b + 1) * RING * RING] + carry
        rank = jnp.sum(hots[b] * before, axis=0, keepdims=True).astype(jnp.int32)
        carry = carry + jnp.sum(hots[b], axis=1, keepdims=True)
        ins, knd, prm = inside[b : b + 1, :], kind[b : b + 1, :], prim[b : b + 1, :]
        spot = sec[b : b + 1, :] * CAP + rank
        slot = jnp.where(ins, (knd * RING + prm) * (HALF * CAP) + spot, -1)
        columns = slice(b * LANES, (b + 1) * LANES)
        place[:, columns] = (iota((place.shape[0], LANES), 0) == slot).astype(F32).astype(BF16)
        marks.append(
            jnp.where(
                iota((2 * RING, LANES), 0) == jnp.where(ins, knd * RING + prm, -1), label[b : b + 1, :], 0.0
            )
        )
        spots.append((iota((LANES, LANES), 0) == me_lane[b : b + 1, :] + spot).astype(F32))
    mine = lax.dot_general(
        jnp.concatenate(marks, axis=1).astype(BF16),
        jnp.concatenate(spots, axis=1).astype(BF16),
        NT,
        preferred_element_type=F32,
    )
    for d in range(2 * RING):
        labels[d] = mine[d : d + 1, :]

    load_pts.wait()
    tile = 256

    def place_tile(i, _):
        columns = pl.ds(pl.multiple_of(i * tile, tile), tile)
        rows = jnp.dot(place[...], pts[:, columns], preferred_element_type=F32).astype(BF16)
        slots[:, :, columns] = rows.reshape(2 * RING, HALF * CAP, tile)
        return 0

    lax.fori_loop(0, width // tile, place_tile, 0)

    pl.semaphore_wait(barrier, 2 * (RING - 1) + n_cent - 1)

    def stage1(route, i):
        to = (pos[route] + i) % RING
        who = {"rows": at(route, to)}
        return (
            pltpu.make_async_remote_copy(
                labels.at[route * RING + to], got_labels.at[route, pos[route]],
                l1_send.at[route, i], l1_recv.at[route, i], who, MESH,
            ),
            pltpu.make_async_remote_copy(
                slots.at[route * RING + to], got.at[route, pos[route]],
                s1_send.at[route, i], s1_recv.at[route, i], who, MESH,
            ),
        )

    for i in ORDER:
        for route in (0, 1):
            for copy in stage1(route, i):
                copy.start()
    for route in (0, 1):
        got_labels[route, pos[route]] = labels[route * RING + pos[route]]
        got[route, pos[route]] = slots[route * RING + pos[route]]

    load_cents.wait()
    chunk = 32

    def smallest(block, low):
        dots = lax.dot_general(block, pts[...], NT, preferred_element_type=F32)
        wide = block.astype(F32)
        norm = jnp.sum(wide * wide, axis=1, keepdims=True)
        return jnp.minimum(low, jnp.min(norm - 2.0 * dots, axis=0, keepdims=True))

    def first_tile(i, low):
        block = cents[pl.ds(i * chunk, chunk)].reshape(chunk * SHARE, width)
        return smallest(block, low)

    none = jnp.full((1, n_pts), jnp.inf, F32)
    best[0] = lax.fori_loop(0, RING * RING // chunk, first_tile, none)
    bests[0, cent] = best[0]

    def norm_tile(i, _):
        rows = pl.ds(pl.multiple_of(i * LANES, LANES), LANES)
        wide = pts[rows, :].astype(F32)
        total = jnp.sum(wide * wide, axis=1, keepdims=True)
        pnorm[:, rows] = jnp.transpose(jnp.broadcast_to(total, (LANES, LANES)))[0:1, :]
        return 0

    lax.fori_loop(0, blocks, norm_tile, 0)

    def across(which, i):
        return pltpu.make_async_remote_copy(
            best.at[which], bests.at[which, cent], c_send.at[which, i], c_recv.at[which, i],
            {"cent": (cent + i) % n_cent}, MESH,
        )

    for route in (0, 1):
        for i in ORDER:
            for copy in stage1(route, i):
                copy.wait_recv()

    def stage2(route, j):
        to = 2 * j + (pos[route] + route) % 2
        me = pos[1 - route]
        return to == me, pltpu.make_async_remote_copy(
            part.at[route, j], parts.at[me],
            s2_send.at[route, j], s2_recv.at[me],
            {"rows": at(1 - route, to)}, MESH,
        )

    for route in (0, 1):
        names = jnp.sum(got_labels[route], axis=0)
        lane = iota((1, LANES), 1)
        target = jnp.where(names > 0.0, ((lane % (HALF * CAP)) // CAP * SHARE).astype(F32) + names - 1.0, -1.0)
        chosen = (iota((HALF * SHARE, LANES), 0).astype(F32) == target).astype(F32)
        counts = jnp.sum(chosen, axis=1, keepdims=True)
        arrived = got[route].reshape(RING * HALF * CAP, width)
        sums = jnp.dot(chosen.astype(BF16), arrived, preferred_element_type=F32)
        part[route, :, :, 0:width] = sums.reshape(HALF, SHARE, width)
        part[route, :, :, width : width + LANES] = jnp.broadcast_to(counts, (HALF * SHARE, LANES)).reshape(
            HALF, SHARE, LANES
        )
        for j in range(HALF):
            mine_too, copy = stage2(route, j)

            @pl.when(jnp.logical_not(mine_too))
            def _():
                copy.start()

            @pl.when(mine_too)
            def _():
                parts[pos[1 - route]] = part[route, j]

    for i in range(1, n_cent):
        across(0, i).start()

    mine_along = jnp.where(par == 0, z, y)
    mine_across = jnp.where(par == 0, y, z)
    for i in range(1, RING):
        src = (mine_along + i) % RING
        pltpu.make_async_remote_copy(
            part.at[0, 0], parts.at[src], s2_send.at[0, 0], s2_recv.at[src], {"rows": row}, MESH
        ).wait_recv()
    total = parts[0]
    for i in range(1, RING):
        total = total + parts[i]
    fresh = (total[:, 0:width] + cents[row].astype(F32)) / (total[:, width : width + 1] + 1.0)
    new[par, mine_across, mine_along // 2] = fresh.astype(BF16)

    def gather1(i):
        to = (mine_along + i) % RING
        who = jnp.where(par == 0, to * RING + y, z * RING + to)
        spot = new.at[par, mine_across, mine_along // 2]
        return pltpu.make_async_remote_copy(
            spot, spot, g1_send.at[i], g1_recv.at[par, mine_along // 2], {"rows": who}, MESH
        )

    for i in ORDER:
        gather1(i).start()

    def group(route, column, q):
        away = pos[1 - route]
        odd = (away + column + route) % 2
        near, far = (0, 2, 6, 4)[q], (1, 7, 3, 5)[q]
        return (away + near + odd * (far - near)) % RING // 2

    def hop(route, kind, d, q):
        sign = 1 - 2 * d
        reach, since = HOPS[kind]
        column = (pos[route] - sign * since) % RING
        spot = new.at[route, column, group(route, column, q)]
        return pltpu.make_async_remote_copy(
            spot, spot, g2_send.at[route, d, kind, q], g2_recv.at[route, d, kind, q],
            {"rows": at(route, (pos[route] + sign * reach) % RING)}, MESH,
        )

    def used(kind, d, q):
        return kind != FAR or (q in (0, 3)) == (d == 0)

    for s, q in WAVE:
        for route in (0, 1):
            if s == 0:
                j = group(route, pos[route], q)
                fetch = pltpu.make_async_remote_copy(
                    new.at[0, 0, 0], new.at[route, pos[route], j], g1_send.at[0], g1_recv.at[route, j],
                    {"rows": row}, MESH,
                )
                if q == 0:
                    pl.when(par != route)(fetch.wait_recv)
                else:
                    fetch.wait_recv()
                for kind in (TWO, ONE):
                    for d in (0, 1):
                        hop(route, kind, d, q).start()
            else:
                for d in (0, 1):
                    hop(route, TWO, d, q).wait_recv()
                    for kind in (FAR, THREE):
                        if used(kind, d, q):
                            hop(route, kind, d, q).start()
    for route in (0, 1):
        for d in (0, 1):
            for q in range(HALF):
                hop(route, ONE, d, q).wait_recv()

    def columns_of(offsets):
        parts_of = [new[route, (pos[route] + k) % RING] for route in (0, 1) for k in offsets]
        return jnp.concatenate(parts_of, axis=0).reshape(2 * len(offsets) * HALF * SHARE, width)

    best[1] = smallest(columns_of((0, 1, 2, 6, 7)), none)
    for q in range(HALF):
        for route in (0, 1):
            for d in (0, 1):
                for kind in (THREE, FAR):
                    if used(kind, d, q):
                        hop(route, kind, d, q).wait_recv()
    best[1] = smallest(columns_of((3, 4, 5)), best[1])
    for i in range(1, n_cent):
        across(1, i).start()
    bests[1, cent] = best[1]
    for which in (0, 1):
        for i in range(1, n_cent):
            across(which, i).wait_recv()

    for route in (0, 1):
        for i in ORDER:
            for copy in stage1(route, i):
                copy.wait_send()
        for j in range(HALF):
            mine_too, copy = stage2(route, j)

            @pl.when(jnp.logical_not(mine_too))
            def _():
                copy.wait_send()

    for i in ORDER:
        gather1(i).wait_send()
    for q in range(HALF):
        for route in (0, 1):
            for d in (0, 1):
                for kind in range(len(HOPS)):
                    if used(kind, d, q):
                        hop(route, kind, d, q).wait_send()
    for which in (0, 1):
        for i in range(1, n_cent):
            across(which, i).wait_send()


def finish(new, bests, pnorm, nearest, updated_hbm, out_sem):
    copies = []
    for p in range(RING):
        copies.append(pltpu.make_async_copy(new.at[0, p], updated_hbm.at[:, p % 2, p // 2, p % 2], out_sem.at[0, p]))
        copies.append(
            pltpu.make_async_copy(new.at[1, p], updated_hbm.at[p // 2, p % 2, :, 1 - p % 2], out_sem.at[1, p])
        )
    for copy in copies:
        copy.start()
    for which in (0, 1):
        low = bests[which, 0]
        for i in range(1, bests.shape[1]):
            low = jnp.minimum(low, bests[which, i])
        nearest[which : which + 1, :] = (pnorm[...] + low) / new.shape[-1]
    for copy in copies:
        copy.wait()


def solution(mesh):
    n_cent = mesh.shape["cent"]

    def per_device(points, centroids, assign):
        n_pts, width = points.shape
        dma = pltpu.SemaphoreType.DMA
        any_space = pl.BlockSpec(memory_space=pltpu.HBM)
        vmem = pl.BlockSpec(memory_space=pltpu.VMEM)
        new, bests, pnorm = pl.pallas_call(
            kernel,
            out_shape=(
                pltpu.VMEM((2, RING, HALF, SHARE, width), BF16),
                pltpu.VMEM((2, n_cent, 1, n_pts), F32),
                pltpu.VMEM((1, n_pts), F32),
            ),
            in_specs=[any_space] * 3,
            out_specs=(vmem,) * 3,
            scratch_shapes=[
                pltpu.VMEM((n_pts // LANES, LANES), jnp.int32),
                pltpu.VMEM((n_pts, width), BF16),
                pltpu.VMEM((RING * RING, SHARE, width), BF16),
                pltpu.VMEM((2 * RING * HALF * CAP, n_pts), BF16),
                pltpu.VMEM((2 * RING, HALF * CAP, width), BF16),
                pltpu.VMEM((2 * RING, 1, LANES), F32),
                pltpu.VMEM((2, RING, HALF * CAP, width), BF16),
                pltpu.VMEM((2, RING, 1, LANES), F32),
                pltpu.VMEM((2, HALF, SHARE, width + LANES), F32),
                pltpu.VMEM((RING, SHARE, width + LANES), F32),
                pltpu.VMEM((2, 1, n_pts), F32),
                dma((3,)),
                dma((2, RING)),
                dma((2, RING)),
                dma((2, RING)),
                dma((2, RING)),
                dma((2, HALF)),
                dma((RING,)),
                dma((RING,)),
                dma((2, HALF)),
                dma((2, 2, len(HOPS), HALF)),
                dma((2, 2, len(HOPS), HALF)),
                dma((2, n_cent)),
                dma((2, n_cent)),
            ],
            compiler_params=pltpu.CompilerParams(
                collective_id=0, has_side_effects=True, vmem_limit_bytes=40 * 1024 * 1024
            ),
        )(
            *(
                pltpu.with_memory_space_constraint(a, pltpu.HBM)
                for a in (
                    points,
                    centroids.reshape(RING * RING, SHARE, width),
                    assign.reshape(n_pts // LANES, LANES),
                )
            )
        )
        nearest, updated = pl.pallas_call(
            finish,
            out_shape=(
                jax.ShapeDtypeStruct((2, n_pts), F32),
                jax.ShapeDtypeStruct((HALF, 2, HALF, 2, SHARE, width), BF16),
            ),
            in_specs=[vmem] * 3,
            out_specs=(vmem, any_space),
            scratch_shapes=[dma((2, RING))],
            compiler_params=pltpu.CompilerParams(vmem_limit_bytes=16 * 1024 * 1024),
        )(new, bests, pnorm)
        return nearest, updated.reshape(RING * RING * SHARE, width)

    return jax.shard_map(
        per_device,
        mesh=mesh,
        in_specs=(P("rows", None), P("cent", None), P("rows")),
        out_specs=(P(None, "rows"), P("cent", None)),
        check_vma=False,
    )
```

```python
import functools

import jax
import jax.numpy as jnp
from jax import lax
from jax.experimental import pallas as pl
from jax.experimental.pallas import tpu as pltpu
from jax.sharding import PartitionSpec as P

MESH = pl.DeviceIdType.MESH
F32 = jnp.float32
BF16 = jnp.bfloat16
RING = 8
HALF = RING // 2
SHARE = 8
CAP = 4
CUTS = 2
LANES = 128
NT = (((1,), (1,)), ((), ()))
ORDER = (4, 3, 5, 2, 6, 1, 7)
ONE, THREE, FAR, TWO = range(4)
HOPS = ((1, 0), (1, 2), (2, 2), (2, 0))
LABELS, STAGE1, STAGE2, COUNTS, GATHER1, GATHER2, ACROSS = range(7)
WAVE = sorted(
    ((s, f, q) for s in range(2) for f in range(CUTS) for q in range(HALF)),
    key=lambda e: 33 * e[0] + 20 * e[1] + 10 * e[2],
)


def iota(shape, dim):
    return lax.broadcasted_iota(jnp.int32, shape, dim)


def kernel(
    points_hbm, cents_hbm, assign_hbm, new, bests, pnorm,
    assigned, pts, cents, place, slots, labels, got, got_labels, part, parts, part_counts, counts_in, best,
    local_sem, sent, l1_recv, s1_recv, s2_recv, g1_recv, two_recv, rest_recv, c_recv,
):
    n_pts, width = points_hbm.shape
    blocks = n_pts // LANES
    cut = width // CUTS
    row = lax.axis_index("rows")
    cent = lax.axis_index("cent")
    z = row // RING
    y = row % RING
    par = (z + y) % 2
    pos = (y, z)
    n_cent = bests.shape[1]

    def awaited(ref, sem):
        return pltpu.make_async_remote_copy(ref, ref, sem, sem, {"rows": row}, MESH)

    def at(route, p):
        return z * RING + p if route == 0 else p * RING + y

    load_assign = pltpu.make_async_copy(assign_hbm, assigned, local_sem.at[2])
    load_assign.start()
    load_pts = pltpu.make_async_copy(points_hbm, pts, local_sem.at[0])
    load_cents = pltpu.make_async_copy(cents_hbm, cents, local_sem.at[1])
    load_pts.start()
    load_cents.start()

    barrier = pltpu.get_barrier_semaphore()
    for route in (0, 1):
        for i in ORDER:
            pl.semaphore_signal(
                barrier, inc=1, device_id={"rows": at(route, (pos[route] + i) % RING)}, device_id_type=MESH
            )
    for i in range(1, n_cent):
        pl.semaphore_signal(barrier, inc=1, device_id={"cent": (cent + i) % n_cent}, device_id_type=MESH)

    load_assign.wait()
    rel = assigned[...] - cent * (RING * RING * SHARE)
    inside = (rel >= 0) & (rel < RING * RING * SHARE)
    owner = jnp.where(inside, rel // SHARE, -1)
    label = jnp.where(inside, rel % SHARE + 1, 0).astype(F32)
    oz = owner // RING
    oy = owner % RING
    kind = (oz + oy) % 2
    prim = jnp.where(kind == 0, oy, oz)
    sec = jnp.where(kind == 0, oz, oy) // 2
    me_lane = jnp.where(kind == 0, y, z) * (HALF * CAP)

    groups = iota((RING * RING, LANES), 0)
    hots = [(groups == owner[b : b + 1, :]).astype(F32) for b in range(blocks)]
    upper = (iota((LANES, LANES), 0) < iota((LANES, LANES), 1)).astype(BF16)
    within = jnp.dot(
        jnp.concatenate(hots, axis=0).astype(BF16), upper, preferred_element_type=F32
    )
    carry = jnp.zeros((RING * RING, 1), F32)
    marks, spots = [], []
    for b in range(blocks):
        before = within[b * RING * RING : (b + 1) * RING * RING] + carry
        rank = jnp.sum(hots[b] * before, axis=0, keepdims=True).astype(jnp.int32)
        carry = carry + jnp.sum(hots[b], axis=1, keepdims=True)
        ins, knd, prm = inside[b : b + 1, :], kind[b : b + 1, :], prim[b : b + 1, :]
        spot = sec[b : b + 1, :] * CAP + rank
        slot = jnp.where(ins, (knd * RING + prm) * (HALF * CAP) + spot, -1)
        columns = slice(b * LANES, (b + 1) * LANES)
        place[:, columns] = (iota((place.shape[0], LANES), 0) == slot).astype(F32).astype(BF16)
        marks.append(
            jnp.where(
                iota((2 * RING, LANES), 0) == jnp.where(ins, knd * RING + prm, -1), label[b : b + 1, :], 0.0
            )
        )
        spots.append((iota((LANES, LANES), 0) == me_lane[b : b + 1, :] + spot).astype(F32))
    mine = lax.dot_general(
        jnp.concatenate(marks, axis=1).astype(BF16),
        jnp.concatenate(spots, axis=1).astype(BF16),
        NT,
        preferred_element_type=F32,
    )
    for d in range(2 * RING):
        labels[d] = mine[d : d + 1, :]

    load_pts.wait()
    tile = 256

    def place_tile(i, _):
        columns = pl.ds(pl.multiple_of(i * tile, tile), tile)
        rows = jnp.dot(place[...], pts[:, columns], preferred_element_type=F32).astype(BF16)
        steps = cut // tile
        slots[i // steps, :, :, pl.ds(pl.multiple_of(i % steps * tile, tile), tile)] = rows.reshape(
            2 * RING, HALF * CAP, tile
        )
        return 0

    def label_copy(route, i):
        to = (pos[route] + i) % RING
        return pltpu.make_async_remote_copy(
            labels.at[route * RING + to], got_labels.at[route, pos[route]],
            sent.at[LABELS], l1_recv.at[0], {"rows": at(route, to)}, MESH,
        )

    def stage1(f, route, i):
        to = (pos[route] + i) % RING
        return pltpu.make_async_remote_copy(
            slots.at[f, route * RING + to], got.at[f, route, pos[route]],
            sent.at[STAGE1], s1_recv.at[f, route], {"rows": at(route, to)}, MESH,
        )

    for f in range(CUTS):
        lax.fori_loop(f * (cut // tile), (f + 1) * (cut // tile), place_tile, 0)
        if f == 0:
            pl.semaphore_wait(barrier, 2 * (RING - 1) + n_cent - 1)
            for i in ORDER:
                for route in (0, 1):
                    label_copy(route, i).start()
        for i in ORDER:
            for route in (0, 1):
                stage1(f, route, i).start()
    for route in (0, 1):
        got_labels[route, pos[route]] = labels[route * RING + pos[route]]
        for f in range(CUTS):
            got[f, route, pos[route]] = slots[f, route * RING + pos[route]]

    load_cents.wait()
    chunk = 32

    def smallest(blocks_of, low):
        dots, norm = 0.0, 0.0
        for f, block in enumerate(blocks_of):
            step = width // len(blocks_of)
            dots += lax.dot_general(
                block, pts[:, f * step : (f + 1) * step], NT, preferred_element_type=F32
            )
            wide = block.astype(F32)
            norm += jnp.sum(wide * wide, axis=1, keepdims=True)
        return jnp.minimum(low, jnp.min(norm - 2.0 * dots, axis=0, keepdims=True))

    def first_tile(i, low):
        block = cents[pl.ds(i * chunk, chunk)].reshape(chunk * SHARE, width)
        return smallest([block], low)

    none = jnp.full((1, n_pts), jnp.inf, F32)
    best[0] = lax.fori_loop(0, RING * RING // chunk, first_tile, none)
    bests[0, cent] = best[0]

    def norm_tile(i, _):
        rows = pl.ds(pl.multiple_of(i * LANES, LANES), LANES)
        wide = pts[rows, :].astype(F32)
        total = jnp.sum(wide * wide, axis=1, keepdims=True)
        pnorm[:, rows] = jnp.transpose(jnp.broadcast_to(total, (LANES, LANES)))[0:1, :]
        return 0

    lax.fori_loop(0, blocks, norm_tile, 0)

    def stage2(f, route, j):
        to = 2 * j + (pos[route] + route) % 2
        me = pos[1 - route]
        return to == me, (
            pltpu.make_async_remote_copy(
                part.at[f, route, j], parts.at[f, me], sent.at[STAGE2], s2_recv.at[f],
                {"rows": at(1 - route, to)}, MESH,
            ),
            pltpu.make_async_remote_copy(
                part_counts.at[route, j], counts_in.at[me], sent.at[COUNTS], s2_recv.at[CUTS],
                {"rows": at(1 - route, to)}, MESH,
            ),
        )

    hot = [None, None]
    for f in range(CUTS):
        for route in (0, 1):
            if f == 0 and route == 0:
                awaited(got_labels.at[:, 0 : RING - 1], l1_recv.at[0]).wait_recv()
            awaited(got.at[f, route, 0 : RING - 1], s1_recv.at[f, route]).wait_recv()
            if f == 0:
                names = jnp.sum(got_labels[route], axis=0)
                lane = iota((1, LANES), 1)
                target = jnp.where(
                    names > 0.0, ((lane % (HALF * CAP)) // CAP * SHARE).astype(F32) + names - 1.0, -1.0
                )
                chosen = (iota((HALF * SHARE, LANES), 0).astype(F32) == target).astype(F32)
                hot[route] = chosen.astype(BF16)
                counts = jnp.sum(chosen, axis=1, keepdims=True)
                part_counts[route] = jnp.broadcast_to(counts, (HALF * SHARE, LANES)).reshape(HALF, SHARE, LANES)
            sums = jnp.dot(
                hot[route], got[f, route].reshape(RING * HALF * CAP, cut), preferred_element_type=F32
            )
            part[f, route] = sums.reshape(HALF, SHARE, cut)
            for j in range(HALF):
                mine_too, copies = stage2(f, route, j)

                @pl.when(jnp.logical_not(mine_too))
                def _():
                    if f == 0:
                        copies[1].start()
                    copies[0].start()

                @pl.when(mine_too)
                def _():
                    if f == 0:
                        counts_in[pos[1 - route]] = part_counts[route, j]
                    parts[f, pos[1 - route]] = part[f, route, j]

    def across(which, i):
        return pltpu.make_async_remote_copy(
            best.at[which], bests.at[which, cent], sent.at[ACROSS], c_recv.at[which],
            {"cent": (cent + i) % n_cent}, MESH,
        )

    for i in range(1, n_cent):
        across(0, i).start()

    mine_along = jnp.where(par == 0, z, y)
    mine_across = jnp.where(par == 0, y, z)

    def gather1(f, i):
        to = (mine_along + i) % RING
        who = jnp.where(par == 0, to * RING + y, z * RING + to)
        spot = new.at[f, par, mine_across, mine_along // 2]
        return pltpu.make_async_remote_copy(
            spot, spot, sent.at[GATHER1], g1_recv.at[f, par, mine_along // 2], {"rows": who}, MESH
        )

    for f in range(CUTS):
        if f == 0:
            awaited(counts_in.at[0 : RING - 1], s2_recv.at[CUTS]).wait_recv()
        awaited(parts.at[f, 0 : RING - 1], s2_recv.at[f]).wait_recv()
        total = parts[f, 0]
        for i in range(1, RING):
            total = total + parts[f, i]
        if f == 0:
            count = counts_in[0]
            for i in range(1, RING):
                count = count + counts_in[i]
            count = count[:, 0:1] + 1.0
        own = cents[row][:, f * cut : (f + 1) * cut].astype(F32)
        new[f, par, mine_across, mine_along // 2] = ((total + own) / count).astype(BF16)
        for i in ORDER:
            gather1(f, i).start()

    def group(route, column, q):
        away = pos[1 - route]
        odd = (away + column + route) % 2
        near, far = (0, 2, 6, 4)[q], (1, 7, 3, 5)[q]
        return (away + near + odd * (far - near)) % RING // 2

    def hop(f, route, kind, d, q):
        sign = 1 - 2 * d
        reach, since = HOPS[kind]
        column = (pos[route] - sign * since) % RING
        spot = new.at[f, route, column, group(route, column, q)]
        return pltpu.make_async_remote_copy(
            spot, spot, sent.at[GATHER2], two_recv.at[f, route, q] if kind == TWO else rest_recv.at[min(kind, 1)],
            {"rows": at(route, (pos[route] + sign * reach) % RING)}, MESH,
        )

    def used(kind, d, q):
        return kind != FAR or (q in (0, 3)) == (d == 0)

    for s, f, q in WAVE:
        for route in (0, 1):
            if s == 0:
                j = group(route, pos[route], q)
                fetch = awaited(new.at[f, route, pos[route], j], g1_recv.at[f, route, j])
                if q == 0:
                    pl.when(par != route)(fetch.wait_recv)
                else:
                    fetch.wait_recv()
                for kind in (TWO, ONE):
                    for d in (0, 1):
                        hop(f, route, kind, d, q).start()
            else:
                awaited(new.at[f, route, 0, 0:2], two_recv.at[f, route, q]).wait_recv()
                for d in (0, 1):
                    for kind in (FAR, THREE):
                        if used(kind, d, q):
                            hop(f, route, kind, d, q).start()
    awaited(new.at[:, :, 0:2], rest_recv.at[0]).wait_recv()

    def columns_of(offsets):
        blocks_of = []
        for f in range(CUTS):
            picked = [new[f, route, (pos[route] + k) % RING] for route in (0, 1) for k in offsets]
            blocks_of.append(jnp.concatenate(picked, axis=0).reshape(2 * len(offsets) * HALF * SHARE, cut))
        return blocks_of

    best[1] = smallest(columns_of((0, 1, 2, 6, 7)), none)
    awaited(new.at[:, :, 0:3], rest_recv.at[1]).wait_recv()
    best[1] = smallest(columns_of((3, 4, 5)), best[1])
    for i in range(1, n_cent):
        across(1, i).start()
    bests[1, cent] = best[1]
    for which in (0, 1):
        awaited(bests.at[which, 0 : n_cent - 1], c_recv.at[which]).wait_recv()

    awaited(got_labels.at[:, 0 : RING - 1], sent.at[LABELS]).wait_send()
    awaited(got.at[:, :, 0 : RING - 1], sent.at[STAGE1]).wait_send()
    awaited(parts.at[:, 0 : RING - 1], sent.at[STAGE2]).wait_send()
    awaited(counts_in.at[0 : RING - 1], sent.at[COUNTS]).wait_send()
    awaited(new.at[:, 0, 0 : RING - 1, 0], sent.at[GATHER1]).wait_send()
    awaited(new.at[:, :, 0 : RING - 1], sent.at[GATHER2]).wait_send()
    awaited(bests.at[:, 0 : n_cent - 1], sent.at[ACROSS]).wait_send()


def finish(new, bests, pnorm, nearest, updated_hbm, out_sem):
    cut = new.shape[-1]
    for f in range(CUTS):
        columns = pl.ds(f * cut, cut)
        for p in range(RING):
            spots = (
                updated_hbm.at[:, p % 2, p // 2, p % 2, :, columns],
                updated_hbm.at[p // 2, p % 2, :, 1 - p % 2, :, columns],
            )
            for route in (0, 1):
                pltpu.make_async_copy(new.at[f, route, p], spots[route], out_sem).start()
    for which in (0, 1):
        low = bests[which, 0]
        for i in range(1, bests.shape[1]):
            low = jnp.minimum(low, bests[which, i])
        nearest[which : which + 1, :] = (pnorm[...] + low) / (CUTS * cut)
    pltpu.make_async_copy(new, new, out_sem).wait()


def solution(mesh):
    n_cent = mesh.shape["cent"]

    def per_device(points, centroids, assign):
        n_pts, width = points.shape
        cut = width // CUTS
        dma = pltpu.SemaphoreType.DMA
        any_space = pl.BlockSpec(memory_space=pltpu.HBM)
        vmem = pl.BlockSpec(memory_space=pltpu.VMEM)
        new, bests, pnorm = pl.pallas_call(
            kernel,
            out_shape=(
                pltpu.VMEM((CUTS, 2, RING, HALF, SHARE, cut), BF16),
                pltpu.VMEM((2, n_cent, 1, n_pts), F32),
                pltpu.VMEM((1, n_pts), F32),
            ),
            in_specs=[any_space] * 3,
            out_specs=(vmem,) * 3,
            scratch_shapes=[
                pltpu.VMEM((n_pts // LANES, LANES), jnp.int32),
                pltpu.VMEM((n_pts, width), BF16),
                pltpu.VMEM((RING * RING, SHARE, width), BF16),
                pltpu.VMEM((2 * RING * HALF * CAP, n_pts), BF16),
                pltpu.VMEM((CUTS, 2 * RING, HALF * CAP, cut), BF16),
                pltpu.VMEM((2 * RING, 1, LANES), F32),
                pltpu.VMEM((CUTS, 2, RING, HALF * CAP, cut), BF16),
                pltpu.VMEM((2, RING, 1, LANES), F32),
                pltpu.VMEM((CUTS, 2, HALF, SHARE, cut), F32),
                pltpu.VMEM((CUTS, RING, SHARE, cut), F32),
                pltpu.VMEM((2, HALF, SHARE, LANES), F32),
                pltpu.VMEM((RING, SHARE, LANES), F32),
                pltpu.VMEM((2, 1, n_pts), F32),
                dma((3,)),
                dma((ACROSS + 1,)),
                dma((1,)),
                dma((CUTS, 2)),
                dma((CUTS + 1,)),
                dma((CUTS, 2, HALF)),
                dma((CUTS, 2, HALF)),
                dma((2,)),
                dma((2,)),
            ],
            compiler_params=pltpu.CompilerParams(
                collective_id=0, has_side_effects=True, vmem_limit_bytes=40 * 1024 * 1024
            ),
        )(
            *(
                pltpu.with_memory_space_constraint(a, pltpu.HBM)
                for a in (
                    points,
                    centroids.reshape(RING * RING, SHARE, width),
                    assign.reshape(n_pts // LANES, LANES),
                )
            )
        )
        nearest, updated = pl.pallas_call(
            finish,
            out_shape=(
                jax.ShapeDtypeStruct((2, n_pts), F32),
                jax.ShapeDtypeStruct((HALF, 2, HALF, 2, SHARE, width), BF16),
            ),
            in_specs=[vmem] * 3,
            out_specs=(vmem, any_space),
            scratch_shapes=[dma],
            compiler_params=pltpu.CompilerParams(vmem_limit_bytes=16 * 1024 * 1024),
        )(new, bests, pnorm)
        return nearest, updated.reshape(RING * RING * SHARE, width)

    return jax.shard_map(
        per_device,
        mesh=mesh,
        in_specs=(P("rows", None), P("cent", None), P("rows")),
        out_specs=(P(None, "rows"), P("cent", None)),
        check_vma=False,
    )
```
